32 devices in a mesh: facet: 8 (over z, core), slab: 4 (over y, x).
Axes of the slice: x: 2, y: 2, z: 4, core: 2. Of those that a mesh axis runs over, the one named last changes fastest.
Arguments:
- facets: float32 [8, 256, 4096], P('facet', 'slab'), may hold values from -20 to 20
- row_taper: float32 [256], P('slab'), may hold values from 0.5 to 2
- col_taper: float32 [4096], replicated, may hold values from 0.5 to 2
- facet_offsets: int32 [8, 2], P('facet'), may hold values from 0 to 32767
- col_offsets: int32 [8], replicated, may hold values from 0 to 32767
- row_offsets: int32 [8, 2], replicated, may hold values from 0 to 32767
Outputs:
- subgrids: float32 [2, 8, 2, 128, 128], P(None, 'facet', None, 'slab')
The draws below stay inside these ranges and needn't reach their ends.
All inputs are finite; a program needn't handle non-finite values.
Results may differ from the reference program's by a relative error of at most 0.0003.
Values sent between devices are 32-bit elements; how exact they have to be, the bound alone decides.
A program may use at most 64 MiB of HBM per device.

```python
import math
import jax
import jax.numpy as jnp
from jax import lax

GRID = 32768
FACET_W = 4096
ROWS_DEV = 64
CONTRIB = 128
SUB_COL = 2
FACETS = 8
COLS = 8
FACET_H = 256


def offset_tables(key):
    base_key = jax.random.fold_in(key, 7301)
    facet_table = jax.random.randint(jax.random.fold_in(base_key, 1), (FACETS, 2), 0, GRID, dtype=jnp.int32)
    column_table = jax.random.randint(jax.random.fold_in(base_key, 2), (COLS,), 0, GRID, dtype=jnp.int32)
    row_table = jax.random.randint(jax.random.fold_in(base_key, 3), (COLS, SUB_COL), 0, GRID, dtype=jnp.int32)
    return (facet_table, column_table, row_table)


def draw_facet_offsets(key, part):
    return offset_tables(key)[0]


def draw_col_offsets(key, part):
    return offset_tables(key)[1]


def draw_row_offsets(key, part):
    return offset_tables(key)[2]


def cosine_tone(positions, frequency):
    product = positions % GRID * (frequency[:, None] % GRID) % GRID
    return jnp.cos(product.astype(jnp.float32) * (2.0 * math.pi / GRID))


def draw_facets(key, part):
    facet_table, column_table, row_table = offset_tables(key)
    draw_keys = [jax.random.fold_in(key, 8101 + number) for number in range(8)]
    white_part = jnp.clip(jax.random.normal(draw_keys[0], (FACETS, FACET_H, FACET_W), jnp.float32), -6.0, 6.0)
    quartic_amp = 8.0
    cubic_amp = 1.5
    edge_amp = 1.5
    shared_column = jax.random.randint(draw_keys[1], (), 0, COLS, dtype=jnp.int32)
    shared_sub = jax.random.randint(draw_keys[2], (), 0, SUB_COL, dtype=jnp.int32)
    shared_row = jax.random.randint(draw_keys[3], (), 0, CONTRIB, dtype=jnp.int32)
    shared_freq = jax.random.randint(draw_keys[4], (), 0, CONTRIB, dtype=jnp.int32)
    own_sub = jax.random.randint(draw_keys[5], (FACETS,), 0, SUB_COL, dtype=jnp.int32)
    own_row = jax.random.randint(draw_keys[6], (FACETS,), 0, CONTRIB, dtype=jnp.int32)
    own_column = jnp.arange(FACETS, dtype=jnp.int32) % COLS
    row_positions = jnp.arange(FACET_H, dtype=jnp.int32)[None, :] + facet_table[:, 0:1]
    col_positions = jnp.arange(FACET_W, dtype=jnp.int32)[None, :] + facet_table[:, 1:2]
    zeros_int = jnp.zeros((FACETS,), jnp.int32)
    shared_rowfreq = zeros_int + row_table[shared_column, shared_sub] + shared_row
    shared_colfreq = zeros_int + column_table[shared_column] + shared_freq
    own_rowfreq = row_table[own_column, own_sub] + own_row
    beyond = CONTRIB - 1 + 5 * (GRID // FACET_W) // 2
    own_colfreq = column_table[own_column] + beyond
    local_row = (jnp.arange(FACET_H, dtype=jnp.int32) % ROWS_DEV).astype(jnp.float32)
    inside = (2.0 * local_row + 1.0) / ROWS_DEV - 1.0
    quartic_term = (35.0 * inside ** 4 - 30.0 * inside ** 2 + 3.0) / 8.0
    cubic_term = (5.0 * inside ** 3 - 3.0 * inside) / 2.0
    shaped_rows = cosine_tone(row_positions, shared_rowfreq) * (quartic_amp * quartic_term + cubic_amp * cubic_term)[None, :]
    planted = shaped_rows[:, :, None] * cosine_tone(col_positions, shared_colfreq)[:, None, :]
    planted = planted + edge_amp * cosine_tone(row_positions, own_rowfreq)[:, :, None] * cosine_tone(col_positions, own_colfreq)[:, None, :]
    return white_part + planted


def shard_levels(own_key, dims, shards, low, largest):
    def one(position, parts):
        draws = jax.random.uniform(jax.random.fold_in(jax.random.fold_in(own_key, 6), position), (parts,), jnp.float32, low / len(shards), largest / len(shards))
        return jnp.repeat(jnp.exp(draws), dims[position] // parts).reshape((-1,) + (1,) * (len(dims) - position - 1))

    gain = one(*shards[0])
    for cut in shards[1:]:
        gain = gain * one(*cut)
    return gain


def setup_inputs(seed: int = 0) -> dict:
    seeds = jax.random.split(jax.random.key(seed), 7)
    return {
        "facets": draw_facets(jax.random.fold_in(seeds[6], 71), 0),
        "row_taper": jnp.clip(jnp.exp(math.log(2.0) - 1.3862944 * jax.random.uniform(seeds[1], (FACET_H,), jnp.float32) ** shard_levels(seeds[1], (FACET_H,), ((0, 4),), -0.2, 0.2)), 0.5, 2.0),
        "col_taper": jnp.clip(jnp.exp(jax.random.uniform(seeds[2], (FACET_W,), jnp.float32, math.log(0.5), math.log(2.0))), 0.5, 2.0),
        "facet_offsets": draw_facet_offsets(jax.random.fold_in(seeds[6], 71), 0),
        "col_offsets": draw_col_offsets(jax.random.fold_in(seeds[6], 71), 0),
        "row_offsets": draw_row_offsets(jax.random.fold_in(seeds[6], 71), 0),
    }


def phase_pair(positions, frequency):
    product = positions[:, None] % GRID * (frequency[..., None, :] % GRID) % GRID
    angles = product.astype(jnp.float32) * (2.0 * math.pi / GRID)
    return (jnp.cos(angles), jnp.sin(angles))

def facet_terms(weighted, row_pos, col_pos, col_offsets, row_offsets):
    highest = lax.Precision.HIGHEST
    frequency = jnp.arange(CONTRIB, dtype=jnp.int32)

    def one_column(column):
        col_cos, col_sin = phase_pair(col_pos, frequency + col_offsets[column])
        tables = jnp.concatenate([col_cos, col_sin], axis=1)
        projected = jnp.dot(weighted, tables, precision=highest, preferred_element_type=jnp.float32)
        real_part = projected[:, :CONTRIB]
        imag_part = -projected[:, CONTRIB:]
        row_cos, row_sin = phase_pair(row_pos, frequency[None, :] + row_offsets[column][:, None])
        sub_real = jnp.einsum('qai,aj->qij', row_cos, real_part, precision=highest) + jnp.einsum('qai,aj->qij', row_sin, imag_part, precision=highest)
        sub_imag = jnp.einsum('qai,aj->qij', row_cos, imag_part, precision=highest) - jnp.einsum('qai,aj->qij', row_sin, real_part, precision=highest)
        return jnp.stack([sub_real, sub_imag])
    stacked = lax.map(one_column, jnp.arange(col_offsets.shape[0], dtype=jnp.int32))
    return jnp.moveaxis(stacked, 0, 1)

def reference(facets, row_taper, col_taper, facet_offsets, col_offsets, row_offsets):
    height = facets.shape[1]
    width = facets.shape[2]
    count = facets.shape[0]

    def add_facet(summed, members):
        image, offsets = members
        weighted = image * row_taper[:, None] * col_taper[None, :]
        row_pos = jnp.arange(height, dtype=jnp.int32) + offsets[0]
        col_pos = jnp.arange(width, dtype=jnp.int32) + offsets[1]
        return (summed + facet_terms(weighted, row_pos, col_pos, col_offsets, row_offsets), None)
    initial = jnp.zeros((2, col_offsets.shape[0], row_offsets.shape[1], CONTRIB, CONTRIB), jnp.float32)
    summed, _ = lax.scan(add_facet, initial, (facets, facet_offsets))
    return summed * (1.0 / math.sqrt(count * height * width))
```

```python
import functools
import math

import jax
import jax.numpy as jnp
from jax import lax
from jax.experimental import pallas as pl
from jax.experimental.pallas import tpu as pltpu
from jax.sharding import PartitionSpec as P

GRID = 32768
CONTRIB = 128
HALF = 256
TURN = 2 * GRID
MESH = pl.DeviceIdType.MESH
F32 = jnp.float32
BF16 = jnp.bfloat16


def cos_sin(steps):
    steps = steps & (TURN - 1)
    quadrant = (steps + TURN // 8) >> 14
    x = (steps - (quadrant << 14)).astype(F32) * (2.0 * math.pi / TURN)
    y = x * x
    s = x + x * y * (-1 / 6 + y * (1 / 120 + y * (-1 / 5040 + y * (1 / 362880))))
    c = 1.0 + y * (-0.5 + y * (1 / 24 + y * (-1 / 720 + y * (1 / 40320))))
    odd = (quadrant & 1) == 1
    cos = jnp.where(odd, s, c)
    sin = jnp.where(odd, c, s)
    cos = jnp.where(((quadrant + 1) & 2) == 2, -cos, cos)
    sin = jnp.where((quadrant & 2) == 2, -sin, sin)
    return cos, sin


def split(x):
    high = x.astype(BF16)
    return high, (x - high.astype(F32)).astype(BF16)


def dot(a, b):
    return jnp.dot(a, b, preferred_element_type=F32)


def kernel(
    groups, slabs, scale,
    facet_ref, row_taper_ref, col_taper_ref, offset_ref, own_offset_ref, col_ref, row_ref,
    out_ref,
    even, odd, outgoing, incoming, offsets, part_out, part_in,
    off_send, off_recv, send, recv, part_send, part_recv,
):
    me = lax.axis_index("facet")
    slab = lax.axis_index("slab")
    rows, width = facet_ref.shape[1], facet_ref.shape[2]
    blocks = width // (2 * HALF)
    subs = row_ref.shape[1]
    pairs = groups // 2
    my_pair = me // 2
    keep = CONTRIB // slabs

    barrier = pltpu.get_barrier_semaphore()
    for d in range(1, groups):
        pl.semaphore_signal(barrier, inc=1, device_id={"facet": lax.rem(me + d, groups)}, device_id_type=MESH)
    for d in range(1, slabs):
        pl.semaphore_signal(barrier, inc=1, device_id={"slab": lax.rem(slab + d, slabs)}, device_id_type=MESH)

    mirror = (
        lax.broadcasted_iota(jnp.int32, (HALF, HALF), 0) + lax.broadcasted_iota(jnp.int32, (HALF, HALF), 1) == HALF - 1
    ).astype(F32).astype(BF16)
    for j in range(blocks):
        lo, mid, hi = 2 * HALF * j, 2 * HALF * j + HALF, 2 * HALF * (j + 1)
        left = facet_ref[0, :, lo:mid] * col_taper_ref[:, lo:mid]
        right = facet_ref[0, :, mid:hi] * col_taper_ref[:, mid:hi]
        left_high, left_low = split(left)
        turned = dot(left_high, mirror) + dot(left_low, mirror)
        band = slice(j * rows, (j + 1) * rows)
        for ref, value in ((even, right + turned), (odd, right - turned)):
            high, low = split(value)
            ref[band, :HALF] = high
            ref[band, HALF : 2 * HALF] = high
            ref[band, 2 * HALF :] = low

    pl.semaphore_wait(barrier, groups - 1 + slabs - 1)

    def offset_copy(peer, home):
        return pltpu.make_async_remote_copy(
            src_ref=offset_ref, dst_ref=offsets.at[home], send_sem=off_send.at[peer], recv_sem=off_recv.at[home],
            device_id={"facet": peer}, device_id_type=MESH,
        )

    def block_copy(peer, home):
        return pltpu.make_async_remote_copy(
            src_ref=outgoing.at[peer], dst_ref=incoming.at[home], send_sem=send.at[peer], recv_sem=recv.at[home],
            device_id={"facet": peer}, device_id_type=MESH,
        )

    def part_copy(peer, home):
        return pltpu.make_async_remote_copy(
            src_ref=part_out.at[peer], dst_ref=part_in.at[home], send_sem=part_send.at[peer], recv_sem=part_recv.at[home],
            device_id={"slab": peer}, device_id_type=MESH,
        )

    for d in range(1, groups):
        offset_copy(lax.rem(me + d, groups), me).start()
    offsets[me] = offset_ref[...]

    order = sorted(range(pairs), key=lambda d: -min(d, pairs - d))
    lane = lax.broadcasted_iota(jnp.int32, (1, 2 * CONTRIB), 1)
    second = lane >= CONTRIB
    twice = 2 * lax.broadcasted_iota(jnp.int32, (HALF, 1), 0) + 1
    centre = 2 * own_offset_ref[0, 1] + 2 * HALF - 1 + 4 * HALF * lax.broadcasted_iota(jnp.int32, (blocks, 1), 0)
    for d in order:
        pair = lax.rem(my_pair + d, pairs)
        frequency = (lane & (CONTRIB - 1)) + jnp.where(second, col_ref[2 * pair + 1], col_ref[2 * pair])
        cos, sin = cos_sin(twice * frequency)
        turn_cos, turn_sin = cos_sin(centre * frequency)
        cos_high, cos_low = split(cos)
        sin_high, sin_low = split(sin)
        evens = dot(even[...], jnp.concatenate([cos_high, cos_low, cos_high], axis=0))
        odds = dot(odd[...], jnp.concatenate([sin_high, sin_low, sin_high], axis=0))
        real = jnp.zeros((rows, 2 * CONTRIB), F32)
        imag = jnp.zeros((rows, 2 * CONTRIB), F32)
        for j in range(blocks):
            e = evens[j * rows : (j + 1) * rows]
            o = odds[j * rows : (j + 1) * rows]
            tc, ts = turn_cos[j : j + 1], turn_sin[j : j + 1]
            real = real + (tc * e - ts * o)
            imag = imag - (ts * e + tc * o)
        for side in range(2):
            span = slice(side * CONTRIB, (side + 1) * CONTRIB)
            outgoing[2 * pair + side, 0] = real[:, span]
            outgoing[2 * pair + side, 1] = imag[:, span]
        if d:
            block_copy(2 * pair, me).start()
            block_copy(2 * pair + 1, me).start()
    twin = me + 1 - 2 * lax.rem(me, 2)
    block_copy(twin, me).start()
    incoming[me] = outgoing[me]

    for d in range(1, groups):
        peer = lax.rem(me + d, groups)
        offset_copy(peer, peer).wait_recv()

    sub = lax.broadcasted_iota(jnp.int32, (subs * CONTRIB, 1), 0)
    row_frequency = sub
    for q in range(subs):
        row_frequency = jnp.where(sub // CONTRIB == q, sub - q * CONTRIB + row_ref[me, q], row_frequency)
    spot = lax.broadcasted_iota(jnp.int32, (1, 2 * rows), 1)
    taper = jnp.concatenate([row_taper_ref[...], row_taper_ref[...]], axis=1)
    tables = []
    for d in order:
        pair = lax.rem(my_pair + pairs - d, pairs)
        base = jnp.where(spot < rows, offsets[2 * pair, :, 0:1], offsets[2 * pair + 1, :, 0:1])
        place = base + jnp.where(spot < rows, spot, spot - rows) + slab * rows
        cos, sin = cos_sin(2 * row_frequency * place)
        high, low = split(jnp.concatenate([cos * taper, sin * taper], axis=1))
        tables.append(jnp.concatenate([high, high, low], axis=1))
    total = None
    for d, table in zip(order, tables):
        pair = lax.rem(my_pair + pairs - d, pairs)
        for side in range(2):
            peer = 2 * pair + side
            if d:
                block_copy(peer, peer).wait_recv()
        if not d:
            block_copy(twin, twin).wait_recv()
        real = incoming[pl.ds(2 * pair, 2), 0].reshape(2 * rows, CONTRIB)
        imag = incoming[pl.ds(2 * pair, 2), 1].reshape(2 * rows, CONTRIB)
        high, low = split(
            jnp.concatenate(
                [jnp.concatenate([real, imag], axis=1), jnp.concatenate([imag, -real], axis=1)], axis=0
            )
        )
        term = dot(table, jnp.concatenate([high, low, high], axis=0))
        total = term if total is None else total + term

    for t in range(slabs):
        for q in range(subs):
            start = q * CONTRIB + t * keep
            part_out[t, q] = total[start : start + keep]
    for d in range(1, slabs):
        part_copy(lax.rem(slab + d, slabs), slab).start()
    result = part_out[slab]
    for d in range(1, slabs):
        peer = lax.rem(slab + d, slabs)
        part_copy(peer, peer).wait_recv()
        result = result + part_in[peer]
    result = result * scale
    out_ref[0, 0] = result[:, :, :CONTRIB]
    out_ref[1, 0] = result[:, :, CONTRIB:]

    for d in range(1, groups):
        peer = lax.rem(me + d, groups)
        offset_copy(peer, me).wait_send()
        block_copy(peer, me).wait_send()
    for d in range(1, slabs):
        part_copy(lax.rem(slab + d, slabs), slab).wait_send()


def solution(mesh):
    groups, slabs = mesh.shape["facet"], mesh.shape["slab"]

    def local(facets, row_taper, col_taper, facet_offsets, col_offsets, row_offsets):
        rows, width = facets.shape[1], facets.shape[2]
        subs = row_offsets.shape[1]
        keep = CONTRIB // slabs
        stacked = width // (2 * HALF) * rows
        scale = 1.0 / math.sqrt(facets.shape[0] * groups * rows * slabs * width)
        vmem = pl.BlockSpec(memory_space=pltpu.VMEM)
        smem = pl.BlockSpec(memory_space=pltpu.SMEM)
        dma = pltpu.SemaphoreType.DMA
        return pl.pallas_call(
            functools.partial(kernel, groups, slabs, scale),
            out_shape=jax.ShapeDtypeStruct((2, 1, subs, keep, CONTRIB), F32),
            in_specs=[vmem, vmem, vmem, vmem, smem, smem, smem],
            out_specs=vmem,
            scratch_shapes=[
                pltpu.VMEM((stacked, 3 * HALF), BF16),
                pltpu.VMEM((stacked, 3 * HALF), BF16),
                pltpu.VMEM((groups, 2, rows, CONTRIB), F32),
                pltpu.VMEM((groups, 2, rows, CONTRIB), F32),
                pltpu.VMEM((groups, 1, 2), jnp.int32),
                pltpu.VMEM((slabs, subs, keep, 2 * CONTRIB), F32),
                pltpu.VMEM((slabs, subs, keep, 2 * CONTRIB), F32),
                dma((groups,)), dma((groups,)), dma((groups,)), dma((groups,)), dma((slabs,)), dma((slabs,)),
            ],
            compiler_params=pltpu.CompilerParams(collective_id=0, has_side_effects=True),
        )(facets, row_taper.reshape(1, rows), col_taper.reshape(1, width), facet_offsets, facet_offsets, col_offsets, row_offsets)

    placed = (P("facet", "slab", None), P("slab"), P(), P("facet", None), P(), P())
    return jax.shard_map(
        local, mesh=mesh, in_specs=placed, out_specs=P(None, "facet", None, "slab", None), check_vma=False
    )
```

```python
import functools
import math

import jax
import jax.numpy as jnp
from jax import lax
from jax.experimental import pallas as pl
from jax.experimental.pallas import tpu as pltpu
from jax.sharding import PartitionSpec as P

GRID = 32768
CONTRIB = 128
HALF = 256
TURN = 2 * GRID
MESH = pl.DeviceIdType.MESH
F32 = jnp.float32
BF16 = jnp.bfloat16


def cos_sin(steps):
    steps = steps & (TURN - 1)
    quadrant = (steps + TURN // 8) >> 14
    x = (steps - (quadrant << 14)).astype(F32) * (2.0 * math.pi / TURN)
    y = x * x
    s = x + x * y * (-1 / 6 + y * (1 / 120 + y * (-1 / 5040 + y * (1 / 362880))))
    c = 1.0 + y * (-0.5 + y * (1 / 24 + y * (-1 / 720 + y * (1 / 40320))))
    odd = (quadrant & 1) == 1
    cos = jnp.where(odd, s, c)
    sin = jnp.where(odd, c, s)
    cos = jnp.where(((quadrant + 1) & 2) == 2, -cos, cos)
    sin = jnp.where((quadrant & 2) == 2, -sin, sin)
    return cos, sin


def split(x):
    high = x.astype(BF16)
    return high, (x - high.astype(F32)).astype(BF16)


def dot(a, b):
    return jnp.dot(a, b, preferred_element_type=F32)


def kernel(
    groups, slabs, scale,
    facet_ref, row_taper_ref, col_taper_ref, offset_ref, own_offset_ref, col_ref, row_ref,
    out_ref,
    even, odd, outgoing, incoming, offsets, part_out, part_in, cross_out, cross_in,
    off_send, off_recv, send, recv, part_send, part_recv, cross_send, cross_recv,
):
    me = lax.axis_index("facet")
    slab = lax.axis_index("slab")
    rows, width = facet_ref.shape[1], facet_ref.shape[2]
    blocks = width // (2 * HALF)
    subs = row_ref.shape[0]
    half = groups // 2
    half_pairs = half // 2
    mine = lax.rem(me, half)
    base = me - mine
    other_base = half - base
    partner = other_base + mine
    my_pair = mine // 2
    keep = CONTRIB // slabs

    barrier = pltpu.get_barrier_semaphore()
    for d in range(1, half):
        pl.semaphore_signal(
            barrier, inc=1, device_id={"facet": base + lax.rem(mine + d, half)}, device_id_type=MESH
        )
    for d in range(1, slabs):
        pl.semaphore_signal(barrier, inc=1, device_id={"slab": lax.rem(slab + d, slabs)}, device_id_type=MESH)
    pl.semaphore_signal(barrier, inc=1, device_id={"facet": partner}, device_id_type=MESH)

    mirror = (
        lax.broadcasted_iota(jnp.int32, (HALF, HALF), 0) + lax.broadcasted_iota(jnp.int32, (HALF, HALF), 1) == HALF - 1
    ).astype(F32).astype(BF16)
    for j in range(blocks):
        lo, mid, hi = 2 * HALF * j, 2 * HALF * j + HALF, 2 * HALF * (j + 1)
        left = facet_ref[0, :, lo:mid] * col_taper_ref[:, lo:mid]
        right = facet_ref[0, :, mid:hi] * col_taper_ref[:, mid:hi]
        left_high, left_low = split(left)
        turned = dot(left_high, mirror) + dot(left_low, mirror)
        band = slice(j * rows, (j + 1) * rows)
        for ref, value in ((even, right + turned), (odd, right - turned)):
            high, low = split(value)
            ref[band, :HALF] = high
            ref[band, HALF : 2 * HALF] = high
            ref[band, 2 * HALF :] = low

    pl.semaphore_wait(barrier, half - 1 + slabs - 1 + 1)

    def offset_copy(peer, home):
        return pltpu.make_async_remote_copy(
            src_ref=offset_ref, dst_ref=offsets.at[home], send_sem=off_send.at[peer], recv_sem=off_recv.at[home],
            device_id={"facet": base + peer}, device_id_type=MESH,
        )

    def block_copy(kind, peer, home):
        return pltpu.make_async_remote_copy(
            src_ref=outgoing.at[kind, peer], dst_ref=incoming.at[kind, home],
            send_sem=send.at[kind, peer], recv_sem=recv.at[kind, home],
            device_id={"facet": base + peer}, device_id_type=MESH,
        )

    def part_copy(kind, peer, home):
        return pltpu.make_async_remote_copy(
            src_ref=part_out.at[kind, peer], dst_ref=part_in.at[kind, home],
            send_sem=part_send.at[kind, peer], recv_sem=part_recv.at[kind, home],
            device_id={"slab": peer}, device_id_type=MESH,
        )

    cross_copy = pltpu.make_async_remote_copy(
        src_ref=cross_out, dst_ref=cross_in, send_sem=cross_send, recv_sem=cross_recv,
        device_id={"facet": partner}, device_id_type=MESH,
    )

    for d in range(1, half):
        offset_copy(lax.rem(mine + d, half), mine).start()
    offsets[mine] = offset_ref[...]

    order = sorted(range(half_pairs), key=lambda d: -min(d, half_pairs - d))
    twin = mine + 1 - 2 * lax.rem(mine, 2)
    lane = lax.broadcasted_iota(jnp.int32, (1, 2 * CONTRIB), 1)
    second = lane >= CONTRIB
    twice = 2 * lax.broadcasted_iota(jnp.int32, (HALF, 1), 0) + 1
    centre = 2 * own_offset_ref[0, 1] + 2 * HALF - 1 + 4 * HALF * lax.broadcasted_iota(jnp.int32, (blocks, 1), 0)
    for kind, first in ((0, other_base), (1, base)):
        for d in order:
            pair = lax.rem(my_pair + d, half_pairs)
            column = first + 2 * pair
            frequency = (lane & (CONTRIB - 1)) + jnp.where(second, col_ref[column + 1], col_ref[column])
            cos, sin = cos_sin(twice * frequency)
            turn_cos, turn_sin = cos_sin(centre * frequency)
            cos_high, cos_low = split(cos)
            sin_high, sin_low = split(sin)
            evens = dot(even[...], jnp.concatenate([cos_high, cos_low, cos_high], axis=0))
            odds = dot(odd[...], jnp.concatenate([sin_high, sin_low, sin_high], axis=0))
            real = jnp.zeros((rows, 2 * CONTRIB), F32)
            imag = jnp.zeros((rows, 2 * CONTRIB), F32)
            for j in range(blocks):
                e = evens[j * rows : (j + 1) * rows]
                o = odds[j * rows : (j + 1) * rows]
                tc, ts = turn_cos[j : j + 1], turn_sin[j : j + 1]
                real = real + (tc * e - ts * o)
                imag = imag - (ts * e + tc * o)
            for side in range(2):
                span = slice(side * CONTRIB, (side + 1) * CONTRIB)
                outgoing[kind, 2 * pair + side, 0] = real[:, span]
                outgoing[kind, 2 * pair + side, 1] = imag[:, span]
            if d:
                block_copy(kind, 2 * pair, mine).start()
                block_copy(kind, 2 * pair + 1, mine).start()
        block_copy(kind, twin, mine).start()
        incoming[kind, mine] = outgoing[kind, mine]

    for d in range(1, half):
        peer = lax.rem(mine + d, half)
        offset_copy(peer, peer).wait_recv()

    sub = lax.broadcasted_iota(jnp.int32, (subs * CONTRIB, 1), 0)
    spot = lax.broadcasted_iota(jnp.int32, (1, 2 * rows), 1)
    taper = jnp.concatenate([row_taper_ref[...], row_taper_ref[...]], axis=1)
    for kind, column in ((0, partner), (1, me)):
        row_frequency = sub
        for q in range(subs):
            row_frequency = jnp.where(sub // CONTRIB == q, sub - q * CONTRIB + row_ref[q, column], row_frequency)
        total = None
        for d in order:
            pair = lax.rem(my_pair + half_pairs - d, half_pairs)
            start = jnp.where(spot < rows, offsets[2 * pair, :, 0:1], offsets[2 * pair + 1, :, 0:1])
            place = start + jnp.where(spot < rows, spot, spot - rows) + slab * rows
            cos, sin = cos_sin(2 * row_frequency * place)
            high, low = split(jnp.concatenate([cos * taper, sin * taper], axis=1))
            table = jnp.concatenate([high, high, low], axis=1)
            if d:
                block_copy(kind, 2 * pair, 2 * pair).wait_recv()
                block_copy(kind, 2 * pair + 1, 2 * pair + 1).wait_recv()
            else:
                block_copy(kind, twin, twin).wait_recv()
            real = incoming[kind, pl.ds(2 * pair, 2), 0].reshape(2 * rows, CONTRIB)
            imag = incoming[kind, pl.ds(2 * pair, 2), 1].reshape(2 * rows, CONTRIB)
            high, low = split(
                jnp.concatenate(
                    [jnp.concatenate([real, imag], axis=1), jnp.concatenate([imag, -real], axis=1)], axis=0
                )
            )
            term = dot(table, jnp.concatenate([high, low, high], axis=0))
            total = term if total is None else total + term
        for t in range(slabs):
            for q in range(subs):
                start = q * CONTRIB + t * keep
                part_out[kind, t, q] = total[start : start + keep]
        for d in range(1, slabs):
            part_copy(kind, lax.rem(slab + d, slabs), slab).start()

    def summed(kind):
        result = part_out[kind, slab]
        for d in range(1, slabs):
            peer = lax.rem(slab + d, slabs)
            part_copy(kind, peer, peer).wait_recv()
            result = result + part_in[kind, peer]
        return result

    cross_out[...] = summed(0)
    cross_copy.start()
    result = summed(1)
    cross_copy.wait_recv()
    result = (result + cross_in[...]) * scale
    out_ref[0, 0] = result[:, :, :CONTRIB]
    out_ref[1, 0] = result[:, :, CONTRIB:]

    for d in range(1, half):
        peer = lax.rem(mine + d, half)
        offset_copy(peer, mine).wait_send()
        for kind in range(2):
            block_copy(kind, peer, mine).wait_send()
    for kind in range(2):
        for d in range(1, slabs):
            part_copy(kind, lax.rem(slab + d, slabs), slab).wait_send()
    cross_copy.wait_send()


def solution(mesh):
    groups, slabs = mesh.shape["facet"], mesh.shape["slab"]

    def local(facets, row_taper, col_taper, facet_offsets, col_offsets, row_offsets):
        rows, width = facets.shape[1], facets.shape[2]
        subs = row_offsets.shape[1]
        keep = CONTRIB // slabs
        half = groups // 2
        stacked = width // (2 * HALF) * rows
        scale = 1.0 / math.sqrt(facets.shape[0] * groups * rows * slabs * width)
        vmem = pl.BlockSpec(memory_space=pltpu.VMEM)
        smem = pl.BlockSpec(memory_space=pltpu.SMEM)
        dma = pltpu.SemaphoreType.DMA
        return pl.pallas_call(
            functools.partial(kernel, groups, slabs, scale),
            out_shape=jax.ShapeDtypeStruct((2, 1, subs, keep, CONTRIB), F32),
            in_specs=[vmem, vmem, vmem, vmem, smem, smem, smem],
            out_specs=vmem,
            scratch_shapes=[
                pltpu.VMEM((stacked, 3 * HALF), BF16),
                pltpu.VMEM((stacked, 3 * HALF), BF16),
                pltpu.VMEM((2, half, 2, rows, CONTRIB), F32),
                pltpu.VMEM((2, half, 2, rows, CONTRIB), F32),
                pltpu.VMEM((half, 1, 2), jnp.int32),
                pltpu.VMEM((2, slabs, subs, keep, 2 * CONTRIB), F32),
                pltpu.VMEM((2, slabs, subs, keep, 2 * CONTRIB), F32),
                pltpu.VMEM((subs, keep, 2 * CONTRIB), F32),
                pltpu.VMEM((subs, keep, 2 * CONTRIB), F32),
                dma((half,)), dma((half,)), dma((2, half)), dma((2, half)), dma((2, slabs)), dma((2, slabs)), dma, dma,
            ],
            compiler_params=pltpu.CompilerParams(collective_id=0, has_side_effects=True),
        )(facets, row_taper.reshape(1, rows), col_taper.reshape(1, width), facet_offsets, facet_offsets, col_offsets, row_offsets.T)

    placed = (P("facet", "slab", None), P("slab"), P(), P("facet", None), P(), P())
    return jax.shard_map(
        local, mesh=mesh, in_specs=placed, out_specs=P(None, "facet", None, "slab", None), check_vma=False
    )
```

```python
import functools
import math

import jax
import jax.numpy as jnp
from jax import lax
from jax.experimental import pallas as pl
from jax.experimental.pallas import tpu as pltpu
from jax.sharding import PartitionSpec as P

GRID = 32768
CONTRIB = 128
HALF = 256
TURN = 2 * GRID
CHUNKS = 4
PIECES = 2
MESH = pl.DeviceIdType.MESH
F32 = jnp.float32
BF16 = jnp.bfloat16


def cos_sin(steps):
    steps = steps & (TURN - 1)
    quadrant = (steps + TURN // 8) >> 14
    x = (steps - (quadrant << 14)).astype(F32) * (2.0 * math.pi / TURN)
    y = x * x
    s = x + x * y * (-1 / 6 + y * (1 / 120 + y * (-1 / 5040 + y * (1 / 362880))))
    c = 1.0 + y * (-0.5 + y * (1 / 24 + y * (-1 / 720 + y * (1 / 40320))))
    odd = (quadrant & 1) == 1
    cos = jnp.where(odd, s, c)
    sin = jnp.where(odd, c, s)
    cos = jnp.where(((quadrant + 1) & 2) == 2, -cos, cos)
    sin = jnp.where((quadrant & 2) == 2, -sin, sin)
    return cos, sin


def split(x):
    high = x.astype(BF16)
    return high, (x - high.astype(F32)).astype(BF16)


def dot(a, b):
    return jnp.dot(a, b, preferred_element_type=F32)


def kernel(
    groups, slabs, scale,
    facet_ref, row_taper_ref, col_taper_ref, offset_ref, own_offset_ref, col_ref, row_ref,
    out_ref,
    facet_buf, out_buf, even, odd, outgoing, incoming, offsets, part_out, part_in, cross_out, cross_in,
    load, store, off_send, off_recv, send, recv, part_send, part_recv, cross_send, cross_recv,
):
    me = lax.axis_index("facet")
    slab = lax.axis_index("slab")
    rows, width = facet_ref.shape[1], facet_ref.shape[2]
    blocks = width // (2 * HALF)
    subs = row_ref.shape[0]
    half = groups // 2
    half_pairs = half // 2
    mine = lax.rem(me, half)
    base = me - mine
    other_base = half - base
    partner = other_base + mine
    my_pair = mine // 2
    keep = CONTRIB // slabs
    share = keep // PIECES
    chunk = width // CHUNKS

    def facet_copy(n):
        span = slice(n * chunk, (n + 1) * chunk)
        return pltpu.make_async_copy(facet_ref.at[0, :, span], facet_buf.at[:, span], load.at[n])

    for n in range(CHUNKS):
        facet_copy(n).start()

    barrier = pltpu.get_barrier_semaphore()
    for d in range(1, half):
        pl.semaphore_signal(
            barrier, inc=1, device_id={"facet": base + lax.rem(mine + d, half)}, device_id_type=MESH
        )
    for d in range(1, slabs):
        pl.semaphore_signal(barrier, inc=1, device_id={"slab": lax.rem(slab + d, slabs)}, device_id_type=MESH)
    pl.semaphore_signal(barrier, inc=1, device_id={"facet": partner}, device_id_type=MESH)

    order = sorted(range(half_pairs), key=lambda d: -min(d, half_pairs - d))
    lane = lax.broadcasted_iota(jnp.int32, (1, 2 * CONTRIB), 1)
    second = lane >= CONTRIB
    twice = 2 * lax.broadcasted_iota(jnp.int32, (HALF, 1), 0) + 1
    centre = 2 * own_offset_ref[0, 1] + 2 * HALF - 1 + 4 * HALF * lax.broadcasted_iota(jnp.int32, (blocks, 1), 0)

    def column_tables(column):
        frequency = (lane & (CONTRIB - 1)) + jnp.where(second, col_ref[column + 1], col_ref[column])
        cos, sin = cos_sin(twice * frequency)
        cos_high, cos_low = split(cos)
        sin_high, sin_low = split(sin)
        return (
            jnp.concatenate([cos_high, cos_low, cos_high], axis=0),
            jnp.concatenate([sin_high, sin_low, sin_high], axis=0),
        ) + cos_sin(centre * frequency)

    tables = column_tables(other_base + 2 * lax.rem(my_pair + order[0], half_pairs))

    mirror = (
        lax.broadcasted_iota(jnp.int32, (HALF, HALF), 0) + lax.broadcasted_iota(jnp.int32, (HALF, HALF), 1) == HALF - 1
    ).astype(F32).astype(BF16)
    for j in range(blocks):
        if j % (blocks // CHUNKS) == 0:
            facet_copy(j // (blocks // CHUNKS)).wait()
        lo, mid, hi = 2 * HALF * j, 2 * HALF * j + HALF, 2 * HALF * (j + 1)
        left = facet_buf[:, lo:mid] * col_taper_ref[:, lo:mid]
        right = facet_buf[:, mid:hi] * col_taper_ref[:, mid:hi]
        left_high, left_low = split(left)
        turned = dot(left_high, mirror) + dot(left_low, mirror)
        band = slice(j * rows, (j + 1) * rows)
        for ref, value in ((even, right + turned), (odd, right - turned)):
            high, low = split(value)
            ref[band, :HALF] = high
            ref[band, HALF : 2 * HALF] = high
            ref[band, 2 * HALF :] = low

    pl.semaphore_wait(barrier, half - 1 + slabs - 1 + 1)

    def offset_copy(peer, home):
        return pltpu.make_async_remote_copy(
            src_ref=offset_ref, dst_ref=offsets.at[home], send_sem=off_send.at[peer], recv_sem=off_recv.at[home],
            device_id={"facet": base + peer}, device_id_type=MESH,
        )

    def block_copy(kind, peer, home):
        return pltpu.make_async_remote_copy(
            src_ref=outgoing.at[kind, peer], dst_ref=incoming.at[kind, home],
            send_sem=send.at[kind, peer], recv_sem=recv.at[kind, home],
            device_id={"facet": base + peer}, device_id_type=MESH,
        )

    def part_copy(kind, piece, peer, home):
        return pltpu.make_async_remote_copy(
            src_ref=part_out.at[kind, peer, piece], dst_ref=part_in.at[kind, home, piece],
            send_sem=part_send.at[kind, peer, piece], recv_sem=part_recv.at[kind, home, piece],
            device_id={"slab": peer}, device_id_type=MESH,
        )

    def cross_copy(piece):
        return pltpu.make_async_remote_copy(
            src_ref=cross_out.at[piece], dst_ref=cross_in.at[piece],
            send_sem=cross_send.at[piece], recv_sem=cross_recv.at[piece],
            device_id={"facet": partner}, device_id_type=MESH,
        )

    for d in range(1, half):
        offset_copy(lax.rem(mine + d, half), mine).start()
    offsets[mine] = offset_ref[...]

    twin = mine + 1 - 2 * lax.rem(mine, 2)
    for kind, first in ((0, other_base), (1, base)):
        for d in order:
            pair = lax.rem(my_pair + d, half_pairs)
            column = first + 2 * pair
            if tables is None:
                tables = column_tables(column)
            cos_table, sin_table, turn_cos, turn_sin = tables
            tables = None
            evens = dot(even[...], cos_table)
            odds = dot(odd[...], sin_table)
            real = jnp.zeros((rows, 2 * CONTRIB), F32)
            imag = jnp.zeros((rows, 2 * CONTRIB), F32)
            for j in range(blocks):
                e = evens[j * rows : (j + 1) * rows]
                o = odds[j * rows : (j + 1) * rows]
                tc, ts = turn_cos[j : j + 1], turn_sin[j : j + 1]
                real = real + (tc * e - ts * o)
                imag = imag - (ts * e + tc * o)
            for side in range(2):
                span = slice(side * CONTRIB, (side + 1) * CONTRIB)
                outgoing[kind, 2 * pair + side, 0] = real[:, span]
                outgoing[kind, 2 * pair + side, 1] = imag[:, span]
            if d:
                block_copy(kind, 2 * pair, mine).start()
                block_copy(kind, 2 * pair + 1, mine).start()
        block_copy(kind, twin, mine).start()
        incoming[kind, mine] = outgoing[kind, mine]

    for d in range(1, half):
        peer = lax.rem(mine + d, half)
        offset_copy(peer, peer).wait_recv()

    sub = lax.broadcasted_iota(jnp.int32, (subs * CONTRIB, 1), 0)
    spot = lax.broadcasted_iota(jnp.int32, (1, 2 * rows), 1)
    taper = jnp.concatenate([row_taper_ref[...], row_taper_ref[...]], axis=1)

    def row_table(column, pair):
        row_frequency = sub
        for q in range(subs):
            row_frequency = jnp.where(sub // CONTRIB == q, sub - q * CONTRIB + row_ref[q, column], row_frequency)
        start = jnp.where(spot < rows, offsets[2 * pair, :, 0:1], offsets[2 * pair + 1, :, 0:1])
        place = start + jnp.where(spot < rows, spot, spot - rows) + slab * rows
        cos, sin = cos_sin(2 * row_frequency * place)
        high, low = split(jnp.concatenate([cos * taper, sin * taper], axis=1))
        return jnp.concatenate([high, high, low], axis=1)

    def row_term(kind, table, pair):
        real = incoming[kind, pl.ds(2 * pair, 2), 0].reshape(2 * rows, CONTRIB)
        imag = incoming[kind, pl.ds(2 * pair, 2), 1].reshape(2 * rows, CONTRIB)
        high, low = split(
            jnp.concatenate([jnp.concatenate([real, imag], axis=1), jnp.concatenate([imag, -real], axis=1)], axis=0)
        )
        return dot(table, jnp.concatenate([high, low, high], axis=0))

    sources = [lax.rem(my_pair + half_pairs - d, half_pairs) for d in order]
    row_tables = [[row_table(column, pair) for pair in sources] for column in (partner, me)]
    totals = []
    for kind in range(2):
        block_copy(kind, twin, twin).wait_recv()
        totals.append(row_term(kind, row_tables[kind][-1], my_pair))
    for kind in range(2):
        total = totals[kind]
        for pair, table in zip(sources[:-1], row_tables[kind]):
            block_copy(kind, 2 * pair, 2 * pair).wait_recv()
            block_copy(kind, 2 * pair + 1, 2 * pair + 1).wait_recv()
            total = total + row_term(kind, table, pair)
        for piece in range(subs * PIECES):
            for t in range(slabs):
                start = piece // PIECES * CONTRIB + t * keep + piece % PIECES * share
                part_out[kind, t, piece] = total[start : start + share]
            for d in range(1, slabs):
                part_copy(kind, piece, lax.rem(slab + d, slabs), slab).start()

    def summed(kind, piece):
        result = part_out[kind, slab, piece]
        for d in range(1, slabs):
            peer = lax.rem(slab + d, slabs)
            part_copy(kind, piece, peer, peer).wait_recv()
            result = result + part_in[kind, peer, piece]
        return result

    for piece in range(subs * PIECES):
        cross_out[piece] = summed(0, piece)
        cross_copy(piece).start()
    sums = [summed(1, piece) for piece in range(subs * PIECES)]
    for piece in range(subs * PIECES):
        cross_copy(piece).wait_recv()
        result = (sums[piece] + cross_in[piece]) * scale
        place = slice(piece % PIECES * share, (piece % PIECES + 1) * share)
        out_buf[0, 0, piece // PIECES, place] = result[:, :CONTRIB]
        out_buf[1, 0, piece // PIECES, place] = result[:, CONTRIB:]
    out_copy = pltpu.make_async_copy(out_buf, out_ref, store)
    out_copy.start()

    for d in range(1, half):
        peer = lax.rem(mine + d, half)
        offset_copy(peer, mine).wait_send()
        for kind in range(2):
            block_copy(kind, peer, mine).wait_send()
    for piece in range(subs * PIECES):
        for kind in range(2):
            for d in range(1, slabs):
                part_copy(kind, piece, lax.rem(slab + d, slabs), slab).wait_send()
        cross_copy(piece).wait_send()
    out_copy.wait()


def solution(mesh):
    groups, slabs = mesh.shape["facet"], mesh.shape["slab"]

    def local(facets, row_taper, col_taper, facet_offsets, col_offsets, row_offsets):
        rows, width = facets.shape[1], facets.shape[2]
        subs = row_offsets.shape[1]
        keep = CONTRIB // slabs
        half = groups // 2
        pieces, share = subs * PIECES, keep // PIECES
        stacked = width // (2 * HALF) * rows
        scale = 1.0 / math.sqrt(facets.shape[0] * groups * rows * slabs * width)
        vmem = pl.BlockSpec(memory_space=pltpu.VMEM)
        smem = pl.BlockSpec(memory_space=pltpu.SMEM)
        dma = pltpu.SemaphoreType.DMA
        return pl.pallas_call(
            functools.partial(kernel, groups, slabs, scale),
            out_shape=jax.ShapeDtypeStruct((2, 1, subs, keep, CONTRIB), F32),
            in_specs=[pl.BlockSpec(memory_space=pltpu.HBM), vmem, vmem, vmem, smem, smem, smem],
            out_specs=pl.BlockSpec(memory_space=pl.ANY),
            scratch_shapes=[
                pltpu.VMEM((rows, width), F32),
                pltpu.VMEM((2, 1, subs, keep, CONTRIB), F32),
                pltpu.VMEM((stacked, 3 * HALF), BF16),
                pltpu.VMEM((stacked, 3 * HALF), BF16),
                pltpu.VMEM((2, half, 2, rows, CONTRIB), F32),
                pltpu.VMEM((2, half, 2, rows, CONTRIB), F32),
                pltpu.VMEM((half, 1, 2), jnp.int32),
                pltpu.VMEM((2, slabs, pieces, share, 2 * CONTRIB), F32),
                pltpu.VMEM((2, slabs, pieces, share, 2 * CONTRIB), F32),
                pltpu.VMEM((pieces, share, 2 * CONTRIB), F32),
                pltpu.VMEM((pieces, share, 2 * CONTRIB), F32),
                dma((CHUNKS,)), dma, dma((half,)), dma((half,)), dma((2, half)), dma((2, half)),
                dma((2, slabs, pieces)), dma((2, slabs, pieces)), dma((pieces,)), dma((pieces,)),
            ],
            compiler_params=pltpu.CompilerParams(
                collective_id=0, has_side_effects=True, vmem_limit_bytes=int(56 * 2**20)
            ),
        )(facets, row_taper.reshape(1, rows), col_taper.reshape(1, width), facet_offsets, facet_offsets, col_offsets, row_offsets.T)

    placed = (P("facet", "slab", None), P("slab"), P(), P("facet", None), P(), P())
    return jax.shard_map(
        local, mesh=mesh, in_specs=placed, out_specs=P(None, "facet", None, "slab", None), check_vma=False
    )
```

```python
import functools
import math

import jax
import jax.numpy as jnp
from jax import lax
from jax.experimental import pallas as pl
from jax.experimental.pallas import tpu as pltpu
from jax.sharding import PartitionSpec as P

GRID = 32768
CONTRIB = 128
HALF = 256
TURN = 2 * GRID
CHUNKS = 4
PIECES = 2
MESH = pl.DeviceIdType.MESH
F32 = jnp.float32
BF16 = jnp.bfloat16


def cos_sin(steps):
    steps = steps & (TURN - 1)
    quadrant = (steps + TURN // 8) >> 14
    x = (steps - (quadrant << 14)).astype(F32) * (2.0 * math.pi / TURN)
    y = x * x
    s = x + x * y * (-1 / 6 + y * (1 / 120 + y * (-1 / 5040 + y * (1 / 362880))))
    c = 1.0 + y * (-0.5 + y * (1 / 24 + y * (-1 / 720 + y * (1 / 40320))))
    odd = (quadrant & 1) == 1
    cos = jnp.where(odd, s, c)
    sin = jnp.where(odd, c, s)
    cos = jnp.where(((quadrant + 1) & 2) == 2, -cos, cos)
    sin = jnp.where((quadrant & 2) == 2, -sin, sin)
    return cos, sin


def split(x):
    high = x.astype(BF16)
    return high, (x - high.astype(F32)).astype(BF16)


def dot(a, b):
    return jnp.dot(a, b, preferred_element_type=F32)


def kernel(
    groups, slabs, scale,
    facet_ref, row_taper_ref, col_taper_ref, offset_ref, own_offset_ref, col_ref, row_ref,
    out_ref,
    facet_buf, out_buf, even, odd, outgoing, incoming, offsets, part_out, part_in, cross_out, cross_in,
    load, store, off_send, off_recv, send, recv, part_send, part_recv, cross_send, cross_recv,
):
    me = lax.axis_index("facet")
    slab = lax.axis_index("slab")
    rows, width = facet_ref.shape[1], facet_ref.shape[2]
    blocks = width // (2 * HALF)
    subs = row_ref.shape[0]
    half = groups // 2
    half_pairs = half // 2
    mine = lax.rem(me, half)
    base = me - mine
    other_base = half - base
    partner = other_base + mine
    my_pair = mine // 2
    keep = CONTRIB // slabs
    share = keep // PIECES
    chunk = width // CHUNKS

    def facet_copy(n):
        span = slice(n * chunk, (n + 1) * chunk)
        return pltpu.make_async_copy(facet_ref.at[0, :, span], facet_buf.at[:, span], load.at[n])

    for n in range(CHUNKS):
        facet_copy(n).start()

    barrier = pltpu.get_barrier_semaphore()
    for d in range(1, half):
        pl.semaphore_signal(
            barrier, inc=1, device_id={"facet": base + lax.rem(mine + d, half)}, device_id_type=MESH
        )
    for d in range(1, slabs):
        pl.semaphore_signal(barrier, inc=1, device_id={"slab": lax.rem(slab + d, slabs)}, device_id_type=MESH)
    pl.semaphore_signal(barrier, inc=1, device_id={"facet": partner}, device_id_type=MESH)

    order = sorted(range(half_pairs), key=lambda d: -min(d, half_pairs - d))
    lane = lax.broadcasted_iota(jnp.int32, (1, 2 * CONTRIB), 1)
    second = lane >= CONTRIB
    twice = 2 * lax.broadcasted_iota(jnp.int32, (HALF, 1), 0) + 1
    centre = 2 * own_offset_ref[0, 1] + 2 * HALF - 1 + 4 * HALF * lax.broadcasted_iota(jnp.int32, (blocks, 1), 0)

    def column_tables(column):
        frequency = (lane & (CONTRIB - 1)) + jnp.where(second, col_ref[column + 1], col_ref[column])
        cos, sin = cos_sin(twice * frequency)
        cos_high, cos_low = split(cos)
        sin_high, sin_low = split(sin)
        return (
            jnp.concatenate([cos_high, cos_low, cos_high], axis=0),
            jnp.concatenate([sin_high, sin_low, sin_high], axis=0),
        ) + cos_sin(centre * frequency)

    tables = column_tables(other_base + 2 * lax.rem(my_pair + order[0], half_pairs))

    mirror = (
        lax.broadcasted_iota(jnp.int32, (HALF, HALF), 0) + lax.broadcasted_iota(jnp.int32, (HALF, HALF), 1) == HALF - 1
    ).astype(F32).astype(BF16)
    for j in range(blocks):
        if j % (blocks // CHUNKS) == 0:
            facet_copy(j // (blocks // CHUNKS)).wait()
        lo, mid, hi = 2 * HALF * j, 2 * HALF * j + HALF, 2 * HALF * (j + 1)
        left = facet_buf[:, lo:mid] * col_taper_ref[:, lo:mid]
        right = facet_buf[:, mid:hi] * col_taper_ref[:, mid:hi]
        left_high, left_low = split(left)
        turned = dot(left_high, mirror) + dot(left_low, mirror)
        band = slice(j * rows, (j + 1) * rows)
        for ref, value in ((even, right + turned), (odd, right - turned)):
            high, low = split(value)
            ref[band, :HALF] = high
            ref[band, HALF : 2 * HALF] = high
            ref[band, 2 * HALF :] = low


    def offset_copy(peer, home):
        return pltpu.make_async_remote_copy(
            src_ref=offset_ref, dst_ref=offsets.at[home], send_sem=off_send.at[peer], recv_sem=off_recv.at[home],
            device_id={"facet": base + peer}, device_id_type=MESH,
        )

    def block_copy(kind, peer, home):
        return pltpu.make_async_remote_copy(
            src_ref=outgoing.at[kind, peer], dst_ref=incoming.at[kind, home],
            send_sem=send.at[kind, peer], recv_sem=recv.at[kind, home],
            device_id={"facet": base + peer}, device_id_type=MESH,
        )

    def part_copy(kind, piece, peer, home):
        return pltpu.make_async_remote_copy(
            src_ref=part_out.at[kind, peer, piece], dst_ref=part_in.at[kind, home, piece],
            send_sem=part_send.at[kind, peer, piece], recv_sem=part_recv.at[kind, home, piece],
            device_id={"slab": peer}, device_id_type=MESH,
        )

    def cross_copy(piece):
        return pltpu.make_async_remote_copy(
            src_ref=cross_out.at[piece], dst_ref=cross_in.at[piece],
            send_sem=cross_send.at[piece], recv_sem=cross_recv.at[piece],
            device_id={"facet": partner}, device_id_type=MESH,
        )

    offsets[mine] = offset_ref[...]

    twin = mine + 1 - 2 * lax.rem(mine, 2)
    for kind, first in ((0, other_base), (1, base)):
        for d in order:
            pair = lax.rem(my_pair + d, half_pairs)
            column = first + 2 * pair
            if tables is None:
                tables = column_tables(column)
            cos_table, sin_table, turn_cos, turn_sin = tables
            tables = None
            evens = dot(even[...], cos_table)
            odds = dot(odd[...], sin_table)
            real = jnp.zeros((rows, 2 * CONTRIB), F32)
            imag = jnp.zeros((rows, 2 * CONTRIB), F32)
            for j in range(blocks):
                e = evens[j * rows : (j + 1) * rows]
                o = odds[j * rows : (j + 1) * rows]
                tc, ts = turn_cos[j : j + 1], turn_sin[j : j + 1]
                real = real + (tc * e - ts * o)
                imag = imag - (ts * e + tc * o)
            for side in range(2):
                span = slice(side * CONTRIB, (side + 1) * CONTRIB)
                outgoing[kind, 2 * pair + side, 0] = real[:, span]
                outgoing[kind, 2 * pair + side, 1] = imag[:, span]
            if not kind and d == order[0]:
                pl.semaphore_wait(barrier, half - 1 + slabs - 1 + 1)
                for e in range(1, half):
                    offset_copy(lax.rem(mine + e, half), mine).start()
            if d:
                block_copy(kind, 2 * pair, mine).start()
                block_copy(kind, 2 * pair + 1, mine).start()
        block_copy(kind, twin, mine).start()
        incoming[kind, mine] = outgoing[kind, mine]

    for d in range(1, half):
        peer = lax.rem(mine + d, half)
        offset_copy(peer, peer).wait_recv()

    sub = lax.broadcasted_iota(jnp.int32, (subs * CONTRIB, 1), 0)
    spot = lax.broadcasted_iota(jnp.int32, (1, 2 * rows), 1)
    taper = jnp.concatenate([row_taper_ref[...], row_taper_ref[...]], axis=1)

    def row_table(column, pair):
        row_frequency = sub
        for q in range(subs):
            row_frequency = jnp.where(sub // CONTRIB == q, sub - q * CONTRIB + row_ref[q, column], row_frequency)
        start = jnp.where(spot < rows, offsets[2 * pair, :, 0:1], offsets[2 * pair + 1, :, 0:1])
        place = start + jnp.where(spot < rows, spot, spot - rows) + slab * rows
        cos, sin = cos_sin(2 * row_frequency * place)
        high, low = split(jnp.concatenate([cos * taper, sin * taper], axis=1))
        return jnp.concatenate([high, high, low], axis=1)

    def row_term(kind, table, pair):
        real = incoming[kind, pl.ds(2 * pair, 2), 0].reshape(2 * rows, CONTRIB)
        imag = incoming[kind, pl.ds(2 * pair, 2), 1].reshape(2 * rows, CONTRIB)
        high, low = split(
            jnp.concatenate([jnp.concatenate([real, imag], axis=1), jnp.concatenate([imag, -real], axis=1)], axis=0)
        )
        return dot(table, jnp.concatenate([high, low, high], axis=0))

    sources = [lax.rem(my_pair + half_pairs - d, half_pairs) for d in order]
    row_tables = [[row_table(column, pair) for pair in sources] for column in (partner, me)]
    totals = []
    for kind in range(2):
        block_copy(kind, twin, twin).wait_recv()
        totals.append(row_term(kind, row_tables[kind][-1], my_pair))
    for kind in range(2):
        total = totals[kind]
        for pair, table in zip(sources[:-1], row_tables[kind]):
            block_copy(kind, 2 * pair, 2 * pair).wait_recv()
            block_copy(kind, 2 * pair + 1, 2 * pair + 1).wait_recv()
            total = total + row_term(kind, table, pair)
        for piece in range(subs * PIECES):
            for t in range(slabs):
                start = piece // PIECES * CONTRIB + t * keep + piece % PIECES * share
                part_out[kind, t, piece] = total[start : start + share]
            for d in range(1, slabs):
                part_copy(kind, piece, lax.rem(slab + d, slabs), slab).start()

    def summed(kind, piece):
        result = part_out[kind, slab, piece]
        for d in range(1, slabs):
            peer = lax.rem(slab + d, slabs)
            part_copy(kind, piece, peer, peer).wait_recv()
            result = result + part_in[kind, peer, piece]
        return result

    for piece in range(subs * PIECES):
        cross_out[piece] = summed(0, piece)
        cross_copy(piece).start()
    sums = [summed(1, piece) for piece in range(subs * PIECES)]
    for piece in range(subs * PIECES):
        cross_copy(piece).wait_recv()
        result = (sums[piece] + cross_in[piece]) * scale
        place = slice(piece % PIECES * share, (piece % PIECES + 1) * share)
        out_buf[0, 0, piece // PIECES, place] = result[:, :CONTRIB]
        out_buf[1, 0, piece // PIECES, place] = result[:, CONTRIB:]
    out_copy = pltpu.make_async_copy(out_buf, out_ref, store)
    out_copy.start()

    for d in range(1, half):
        peer = lax.rem(mine + d, half)
        offset_copy(peer, mine).wait_send()
        for kind in range(2):
            block_copy(kind, peer, mine).wait_send()
    for piece in range(subs * PIECES):
        for kind in range(2):
            for d in range(1, slabs):
                part_copy(kind, piece, lax.rem(slab + d, slabs), slab).wait_send()
        cross_copy(piece).wait_send()
    out_copy.wait()


def solution(mesh):
    groups, slabs = mesh.shape["facet"], mesh.shape["slab"]

    def local(facets, row_taper, col_taper, facet_offsets, col_offsets, row_offsets):
        rows, width = facets.shape[1], facets.shape[2]
        subs = row_offsets.shape[1]
        keep = CONTRIB // slabs
        half = groups // 2
        pieces, share = subs * PIECES, keep // PIECES
        stacked = width // (2 * HALF) * rows
        scale = 1.0 / math.sqrt(facets.shape[0] * groups * rows * slabs * width)
        vmem = pl.BlockSpec(memory_space=pltpu.VMEM)
        smem = pl.BlockSpec(memory_space=pltpu.SMEM)
        dma = pltpu.SemaphoreType.DMA
        return pl.pallas_call(
            functools.partial(kernel, groups, slabs, scale),
            out_shape=jax.ShapeDtypeStruct((2, 1, subs, keep, CONTRIB), F32),
            in_specs=[pl.BlockSpec(memory_space=pltpu.HBM), vmem, vmem, vmem, smem, smem, smem],
            out_specs=pl.BlockSpec(memory_space=pl.ANY),
            scratch_shapes=[
                pltpu.VMEM((rows, width), F32),
                pltpu.VMEM((2, 1, subs, keep, CONTRIB), F32),
                pltpu.VMEM((stacked, 3 * HALF), BF16),
                pltpu.VMEM((stacked, 3 * HALF), BF16),
                pltpu.VMEM((2, half, 2, rows, CONTRIB), F32),
                pltpu.VMEM((2, half, 2, rows, CONTRIB), F32),
                pltpu.VMEM((half, 1, 2), jnp.int32),
                pltpu.VMEM((2, slabs, pieces, share, 2 * CONTRIB), F32),
                pltpu.VMEM((2, slabs, pieces, share, 2 * CONTRIB), F32),
                pltpu.VMEM((pieces, share, 2 * CONTRIB), F32),
                pltpu.VMEM((pieces, share, 2 * CONTRIB), F32),
                dma((CHUNKS,)), dma, dma((half,)), dma((half,)), dma((2, half)), dma((2, half)),
                dma((2, slabs, pieces)), dma((2, slabs, pieces)), dma((pieces,)), dma((pieces,)),
            ],
            compiler_params=pltpu.CompilerParams(
                collective_id=0, has_side_effects=True, vmem_limit_bytes=int(56 * 2**20)
            ),
        )(facets, row_taper.reshape(1, rows), col_taper.reshape(1, width), facet_offsets, facet_offsets, col_offsets, row_offsets.T)

    placed = (P("facet", "slab", None), P("slab"), P(), P("facet", None), P(), P())
    return jax.shard_map(
        local, mesh=mesh, in_specs=placed, out_specs=P(None, "facet", None, "slab", None), check_vma=False
    )
```
